16 devices in a mesh: dp: 2 (over z), fsdp: 8 (over y, x, core).
Axes of the slice: x: 2, y: 2, z: 2, core: 2. Of those that a mesh axis runs over, the one named last changes fastest.
Arguments:
- x_in: bfloat16 [16, 1024, 768], P(('dp', 'fsdp'))
- positions: int32 [16, 1024], P(('dp', 'fsdp'))
- segments: int32 [16, 1024], P(('dp', 'fsdp'))
- rel_bias: float32 [32, 12], replicated
- gain_attn: float32 [768], replicated
- gain_mlp: float32 [768], replicated
- w_q: bfloat16 [768, 768], P('fsdp')
- w_k: bfloat16 [768, 768], P('fsdp')
- w_v: bfloat16 [768, 768], P('fsdp')
- w_o: bfloat16 [768, 768], P('fsdp')
- w_i0: bfloat16 [768, 2048], P('fsdp')
- w_i1: bfloat16 [768, 2048], P('fsdp')
- w_f: bfloat16 [2048, 768], P('fsdp')
- grad_out: bfloat16 [16, 1024, 768], P(('dp', 'fsdp'))
Outputs:
- output 1: bfloat16 [16, 1024, 768], P(('dp', 'fsdp'))
- output 2: float32 [32, 12], replicated
- output 3: float32 [768], replicated
- output 4: float32 [768], replicated
- output 5: bfloat16 [768, 768], P('fsdp')
- output 6: bfloat16 [768, 768], P('fsdp')
- output 7: bfloat16 [768, 768], P('fsdp')
- output 8: bfloat16 [768, 768], P('fsdp')
- output 9: bfloat16 [768, 2048], P('fsdp')
- output 10: bfloat16 [768, 2048], P('fsdp')
- output 11: bfloat16 [2048, 768], P('fsdp')
All inputs are finite; a program needn't handle non-finite values.
Results may differ from the reference program's by a relative error of at most 0.0190183.
Values are sent between devices in bfloat16 or wider.
A program may use at most 1 GiB of HBM per device.

```python
import jax
import jax.numpy as jnp
from jax import lax

BATCH_ROWS = 16
SEQ_LEN = 1024
D_MODEL = 768
HEADS = 12
HEAD_DIM = 64
FF_DIM = 2048
REL_CLASSES = 32
HALF_CLASSES = REL_CLASSES // 2
EXACT_RANGE = HALF_CLASSES // 2
THRESHOLDS = (12, 16, 23, 32, 46, 64, 91)
EPSILON = 1e-6
NEG_BIG = -1e9


def draw_segments(key):
    margin = SEQ_LEN // 8
    cuts = jax.random.randint(key, (BATCH_ROWS, 2), margin, SEQ_LEN - margin + 1)
    first_cut = jnp.min(cuts, axis=1, keepdims=True)
    second_cut = jnp.max(cuts, axis=1, keepdims=True)
    index = jnp.arange(SEQ_LEN, dtype=jnp.int32)[None, :]
    segments = (index >= first_cut).astype(jnp.int32) + (index >= second_cut).astype(jnp.int32)
    start = jnp.where(segments == 0, 0, jnp.where(segments == 1, first_cut, second_cut))
    positions = (index - start).astype(jnp.int32)
    return positions, segments


def setup_inputs(seed: int = 0) -> dict:
    keys = jax.random.split(jax.random.key(seed), 14)
    width = HEADS * HEAD_DIM
    act_shape = (BATCH_ROWS, SEQ_LEN, D_MODEL)
    score_scale = D_MODEL ** -0.5 * (2.0 / HEAD_DIM) ** 0.25

    def draw_normal(key, shape, scale):
        return jax.random.normal(key, shape, jnp.float32) * scale

    x_in = draw_normal(keys[0], act_shape, 1.0).astype(jnp.bfloat16)
    positions, segments = draw_segments(keys[1])
    rel_bias = draw_normal(keys[2], (REL_CLASSES, HEADS), 1.0)
    gain_attn = 1.0 + draw_normal(keys[3], (D_MODEL,), 0.4)
    gain_mlp = 1.0 + draw_normal(keys[4], (D_MODEL,), 0.4)
    w_q = draw_normal(keys[5], (D_MODEL, width), score_scale).astype(jnp.bfloat16)
    w_k = draw_normal(keys[6], (D_MODEL, width), score_scale).astype(jnp.bfloat16)
    w_v = draw_normal(keys[7], (D_MODEL, width), D_MODEL ** -0.5).astype(jnp.bfloat16)
    w_o = draw_normal(keys[8], (width, D_MODEL), 2.0 * width ** -0.5).astype(jnp.bfloat16)
    w_i0 = draw_normal(keys[9], (D_MODEL, FF_DIM), D_MODEL ** -0.5).astype(jnp.bfloat16)
    w_i1 = draw_normal(keys[10], (D_MODEL, FF_DIM), D_MODEL ** -0.5).astype(jnp.bfloat16)
    w_f = draw_normal(keys[11], (FF_DIM, D_MODEL), 2.0 * FF_DIM ** -0.5).astype(jnp.bfloat16)
    grad_out = draw_normal(keys[12], act_shape, 1.0).astype(jnp.bfloat16)
    return {'x_in': x_in, 'positions': positions, 'segments': segments, 'rel_bias': rel_bias,
            'gain_attn': gain_attn, 'gain_mlp': gain_mlp, 'w_q': w_q, 'w_k': w_k, 'w_v': w_v,
            'w_o': w_o, 'w_i0': w_i0, 'w_i1': w_i1, 'w_f': w_f, 'grad_out': grad_out}


def mat(left, right):
    return jnp.dot(left.astype(jnp.float32), right.astype(jnp.float32))


def rms_norm(values, gain):
    inv_rms = lax.rsqrt(jnp.mean(values * values, axis=-1, keepdims=True) + EPSILON)
    return (values * inv_rms * gain).astype(jnp.bfloat16)


def rel_class(pos_row):
    offset = pos_row[None, :] - pos_row[:, None]
    distance = jnp.abs(offset)
    magnitude = jnp.minimum(distance, EXACT_RANGE)
    for bound in THRESHOLDS:
        magnitude = magnitude + (distance >= bound).astype(jnp.int32)
    return magnitude + HALF_CLASSES * (offset > 0).astype(jnp.int32)


def attend_row(q_row, k_row, v_row, pos_row, seg_row, rel_bias):
    scores = jnp.einsum('qhd,khd->hqk', q_row.astype(jnp.float32), k_row.astype(jnp.float32))
    bias = jnp.transpose(rel_bias[rel_class(pos_row)], (2, 0, 1))
    same_seg = seg_row[:, None] == seg_row[None, :]
    scores = scores + bias + jnp.where(same_seg, 0.0, NEG_BIG)
    attn_prob = jax.nn.softmax(scores, axis=-1)
    context = jnp.einsum('hqk,khd->qhd', attn_prob.astype(jnp.bfloat16).astype(jnp.float32), v_row.astype(jnp.float32))
    return context.astype(jnp.bfloat16)


def layer(x_in, positions, segments, param_set):
    rel_bias, gain_attn, gain_mlp, w_q, w_k, w_v, w_o, w_i0, w_i1, w_f = param_set
    rows, seq_len, width = x_in.shape
    heads = rel_bias.shape[1]
    x_float = x_in.astype(jnp.float32).reshape(rows * seq_len, width)
    normed = rms_norm(x_float, gain_attn)
    q_all = mat(normed, w_q).astype(jnp.bfloat16).reshape(rows, seq_len, heads, -1)
    k_all = mat(normed, w_k).astype(jnp.bfloat16).reshape(rows, seq_len, heads, -1)
    v_all = mat(normed, w_v).astype(jnp.bfloat16).reshape(rows, seq_len, heads, -1)
    row_attend = jax.checkpoint(lambda row_args: attend_row(row_args[0], row_args[1], row_args[2], row_args[3], row_args[4], rel_bias))
    context = lax.map(row_attend, (q_all, k_all, v_all, positions, segments))
    context = context.reshape(rows * seq_len, -1)
    hidden = (x_float + mat(context, w_o)).astype(jnp.bfloat16)
    h_float = hidden.astype(jnp.float32)
    mlp_in = rms_norm(h_float, gain_mlp)
    hidden_act = (jax.nn.silu(mat(mlp_in, w_i0)) * mat(mlp_in, w_i1)).astype(jnp.bfloat16)
    y_out = (h_float + mat(hidden_act, w_f)).astype(jnp.bfloat16)
    return y_out.reshape(rows, seq_len, width)


def reference(x_in, positions, segments, rel_bias, gain_attn, gain_mlp, w_q, w_k, w_v, w_o, w_i0, w_i1, w_f, grad_out):
    param_set = (rel_bias, gain_attn, gain_mlp, w_q, w_k, w_v, w_o, w_i0, w_i1, w_f)
    y_out, pull_back = jax.vjp(lambda params_in: layer(x_in, positions, segments, params_in), param_set)
    grads = pull_back(grad_out)[0]
    return (y_out, grads[0], grads[1], grads[2], grads[3], grads[4], grads[5], grads[6], grads[7], grads[8], grads[9])
```

```python
import jax
import jax.numpy as jnp
import numpy as np
from jax import lax
from jax.experimental import pallas as pl
from jax.experimental.pallas import tpu as pltpu
from jax.sharding import PartitionSpec as P

EPSILON = 1e-6
NEG_BIG = -1e9
CLASSES = 32
HALF_CLASSES = 16
EXACT_RANGE = 8
THRESHOLDS = (12, 16, 23, 32, 46, 64, 91)
ROW_AXES = ('dp', 'fsdp')
LANES = 128
QT = 256
KC = 256
SK = 64
HB = 4
HD = 64
NKS = KC // SK
NQS = QT // LANES
FT = 256

NT = (((1,), (1,)), ((), ()))
NN = (((1,), (0,)), ((), ()))
AXIS_BIT = {'c': 1, 'x': 2, 'y': 4, 'z': 8}


def class_index(pos_q, pos_k, seg_q, seg_k):
    offset = pos_k - pos_q
    distance = jnp.abs(offset)
    magnitude = jnp.minimum(distance, EXACT_RANGE)
    for bound in THRESHOLDS:
        magnitude = magnitude + (distance >= bound).astype(jnp.int32)
    rel_cls = magnitude + HALF_CLASSES * (offset > 0).astype(jnp.int32)
    return rel_cls + CLASSES * (seg_q != seg_k).astype(jnp.int32)


def bias_table(rel_bias):
    both = jnp.concatenate([rel_bias, rel_bias + NEG_BIG], axis=0).T
    heads = both.shape[0]
    tab = jnp.pad(both, ((0, 0), (0, LANES - 2 * CLASSES)))
    return jnp.broadcast_to(tab[:, None, :], (heads, 8, LANES))


def head_lanes(x, h):
    lane = lax.broadcasted_iota(jnp.int32, x.shape, 1)
    return jnp.where((lane >= HD * h) & (lane < HD * (h + 1)), x, jnp.zeros_like(x))


def fwd_kernel(act_ref, lo_ref, hi_ref, tabs_ref, q_ref, k_ref, v_ref, idx_ref, tab_ref,
               ctx_ref, ctx32_ref, p_ref, vt_scr, m_scr, l_scr, o_scr):
    g = pl.program_id(0)
    t = pl.program_id(1)
    S = k_ref.shape[0]

    @pl.when(t == 0)
    def _():
        for j in range(HB // 2):
            vt_scr[j * LANES:(j + 1) * LANES, :] = v_ref[:, j * LANES:(j + 1) * LANES].astype(jnp.float32).T.astype(jnp.bfloat16)

    m_scr[...] = jnp.full(m_scr.shape, -jnp.inf, jnp.float32)
    l_scr[...] = jnp.zeros_like(l_scr)
    o_scr[...] = jnp.zeros_like(o_scr)

    for c in range(S // KC):
        @pl.when(act_ref[c, t] != 0)
        def _(c=c):
            ks = slice(c * KC, (c + 1) * KC)
            for h in range(HB):
                js = slice((h // 2) * LANES, (h // 2 + 1) * LANES)
                p_ref[h, ks, :] = lax.dot_general(head_lanes(k_ref[ks, js], h % 2), q_ref[:, js], NT, preferred_element_type=jnp.float32)
            for a in range(NKS):
                for b in range(NQS):
                    lo = lo_ref[c * NKS + a, t * NQS + b]
                    hi = hi_ref[c * NKS + a, t * NQS + b]
                    rs = slice(c * KC + a * SK, c * KC + (a + 1) * SK)
                    cs = slice(b * LANES, (b + 1) * LANES)
                    gc = pl.ds(pl.multiple_of(t * QT + b * LANES, LANES), LANES)

                    @pl.when(lo == hi)
                    def _():
                        for h in range(HB):
                            s = p_ref[h, rs, cs] + tabs_ref[g * HB + h, lo]
                            p_ref[h, rs, cs] = s
                            m_scr[h, :, cs] = jnp.maximum(m_scr[h, :, cs], jnp.max(s.reshape(SK // 8, 8, LANES), axis=0))

                    @pl.when(lo != hi)
                    def _():
                        for r in range(SK // 8):
                            r8 = slice(c * KC + a * SK + r * 8, c * KC + a * SK + r * 8 + 8)
                            ix = idx_ref[r8, gc]
                            for h in range(HB):
                                bias = jnp.take_along_axis(tab_ref[h], ix, axis=1, mode='promise_in_bounds')
                                s = p_ref[h, r8, cs] + bias
                                p_ref[h, r8, cs] = s
                                m_scr[h, :, cs] = jnp.maximum(m_scr[h, :, cs], s)

    for h in range(HB):
        m_scr[h] = jnp.broadcast_to(jnp.max(m_scr[h], axis=0, keepdims=True), (8, QT))
    for c in range(S // KC):
        @pl.when(act_ref[c, t] != 0)
        def _(c=c):
            ks = slice(c * KC, (c + 1) * KC)
            for h in range(HB):
                e = jnp.exp(p_ref[h, ks, :].reshape(KC // 8, 8, QT) - m_scr[h])
                p_ref[h, ks, :] = e.reshape(KC, QT)
                l_scr[h] += jnp.sum(e, axis=0)
    for h in range(HB):
        l_scr[h] = jnp.broadcast_to(1.0 / jnp.sum(l_scr[h], axis=0, keepdims=True), (8, QT))
    for c in range(S // KC):
        @pl.when(act_ref[c, t] != 0)
        def _(c=c):
            ks = slice(c * KC, (c + 1) * KC)
            for h in range(HB):
                pr = (p_ref[h, ks, :].reshape(KC // 8, 8, QT) * l_scr[h]).reshape(KC, QT)
                p_ref[h, ks, :] = pr
                hs = slice(h * HD, (h + 1) * HD)
                o_scr[hs, :] += lax.dot_general(vt_scr[hs, ks], pr.astype(jnp.bfloat16), NN, preferred_element_type=jnp.float32)
    o = o_scr[...].T
    ctx32_ref[...] = o
    ctx_ref[...] = o.astype(jnp.bfloat16)


def attn_fwd(qkv, idx_t, tab, tabs, act, lo, hi):
    S = qkv.shape[0]
    heads = tab.shape[0]
    G = heads // HB
    BW = HB * HD
    W = heads * HD
    gs = pltpu.PrefetchScalarGridSpec(
        num_scalar_prefetch=4,
        grid=(G, S // QT),
        in_specs=[
            pl.BlockSpec((QT, BW), lambda p, t, *_: (t, p)),
            pl.BlockSpec((S, BW), lambda p, t, *_: (0, G + p)),
            pl.BlockSpec((S, BW), lambda p, t, *_: (0, 2 * G + p)),
            pl.BlockSpec((S, S), lambda p, t, *_: (0, 0)),
            pl.BlockSpec((HB, 8, LANES), lambda p, t, *_: (p, 0, 0)),
        ],
        out_specs=[
            pl.BlockSpec((QT, BW), lambda p, t, *_: (t, p)),
            pl.BlockSpec((QT, BW), lambda p, t, *_: (t, p)),
            pl.BlockSpec((HB, S, QT), lambda p, t, *_: (p, 0, t)),
        ],
        scratch_shapes=[pltpu.VMEM((BW, S), jnp.bfloat16), pltpu.VMEM((HB, 8, QT), jnp.float32),
                        pltpu.VMEM((HB, 8, QT), jnp.float32), pltpu.VMEM((BW, QT), jnp.float32)],
    )
    return pl.pallas_call(
        fwd_kernel,
        grid_spec=gs,
        out_shape=[
            jax.ShapeDtypeStruct((S, W), jnp.bfloat16),
            jax.ShapeDtypeStruct((S, W), jnp.float32),
            jax.ShapeDtypeStruct((heads, S, S), jnp.float32),
        ],
        cost_estimate=pl.CostEstimate(flops=40_000_000_000, bytes_accessed=60_000_000, transcendentals=0),
        name="attn_fwd",
    )(act, lo, hi, tabs, qkv, qkv, qkv, idx_t, tab)


def bwd_kernel(act_ref, lo_ref, hi_ref, q_ref, k_ref, v_ref, dc_ref, ctx32_ref, p_ref, idx_ref,
               dq_ref, dk_ref, dv_ref, db_ref, kt_scr, dk_acc, dv_acc, dqt_acc, dlt_scr, ds_scr):
    t = pl.program_id(1)
    S = k_ref.shape[0]

    @pl.when(t == 0)
    def _():
        for j in range(HB // 2):
            js = slice(j * LANES, (j + 1) * LANES)
            kt_scr[js, :] = k_ref[:, js].astype(jnp.float32).T.astype(jnp.bfloat16)
        dk_acc[...] = jnp.zeros_like(dk_acc)
        dv_acc[...] = jnp.zeros_like(dv_acc)
        db_ref[...] = jnp.zeros_like(db_ref)

    dqt_acc[...] = jnp.zeros_like(dqt_acc)
    for j in range(HB // 2):
        js = slice(j * LANES, (j + 1) * LANES)
        prod_t = (ctx32_ref[:, js] * dc_ref[:, js].astype(jnp.float32)).T
        for h in range(2):
            d = jnp.sum(prod_t[HD * h:HD * (h + 1), :], axis=0, keepdims=True)
            dlt_scr[2 * j + h] = jnp.broadcast_to(d, (8, QT))

    for c in range(S // KC):
        @pl.when(act_ref[c, t] != 0)
        def _(c=c):
            ks = slice(c * KC, (c + 1) * KC)
            for h in range(HB):
                js = slice((h // 2) * LANES, (h // 2 + 1) * LANES)
                hs = slice(h * HD, (h + 1) * HD)
                dp = lax.dot_general(head_lanes(v_ref[ks, js], h % 2), dc_ref[:, js], NT, preferred_element_type=jnp.float32)
                pr = p_ref[h, ks, :]
                ds = pr * (dp.reshape(KC // 8, 8, QT) - dlt_scr[h]).reshape(KC, QT)
                ds_scr[h] = ds
                ds16 = ds.astype(jnp.bfloat16)
                dv_acc[ks, js] += lax.dot_general(pr.astype(jnp.bfloat16), head_lanes(dc_ref[:, js], h % 2), NN, preferred_element_type=jnp.float32)
                dk_acc[ks, js] += lax.dot_general(ds16, head_lanes(q_ref[:, js], h % 2), NN, preferred_element_type=jnp.float32)
                dqt_acc[hs, :] += lax.dot_general(kt_scr[hs, ks], ds16, NN, preferred_element_type=jnp.float32)

            for a in range(NKS):
                for b in range(NQS):
                    lo = lo_ref[c * NKS + a, t * NQS + b]
                    hi = hi_ref[c * NKS + a, t * NQS + b]
                    rs = slice(a * SK, (a + 1) * SK)
                    cs = slice(b * LANES, (b + 1) * LANES)
                    gr = slice(c * KC + a * SK, c * KC + (a + 1) * SK)
                    gc = pl.ds(pl.multiple_of(t * QT + b * LANES, LANES), LANES)

                    @pl.when(lo == hi)
                    def _():
                        for h in range(HB):
                            db_ref[lo, h] += jnp.sum(ds_scr[h, rs, cs].reshape(SK // 8, 8, LANES), axis=0)

                    @pl.when(lo < hi)
                    def _():
                        @pl.loop(lo, hi + 1)
                        def _(cls):
                            eq = idx_ref[gr, gc] == cls
                            for h in range(HB):
                                x = jnp.where(eq, ds_scr[h, rs, cs], 0.0).reshape(SK // 8, 8, LANES)
                                db_ref[cls, h] += jnp.sum(x, axis=0)

    dq_ref[...] = dqt_acc[...].T.astype(jnp.bfloat16)

    @pl.when(t == pl.num_programs(1) - 1)
    def _():
        dk_ref[...] = dk_acc[...].astype(jnp.bfloat16)
        dv_ref[...] = dv_acc[...].astype(jnp.bfloat16)


def attn_bwd(qkv, d_ctx, ctx32, probs, idx_t, act, lo, hi, first, count):
    S = qkv.shape[0]
    heads = probs.shape[0]
    G = heads // HB
    BW = HB * HD
    W = count * BW
    f = first
    gs = pltpu.PrefetchScalarGridSpec(
        num_scalar_prefetch=3,
        grid=(count, S // QT),
        in_specs=[
            pl.BlockSpec((QT, BW), lambda p, t, *_: (t, f + p)),
            pl.BlockSpec((S, BW), lambda p, t, *_: (0, G + f + p)),
            pl.BlockSpec((S, BW), lambda p, t, *_: (0, 2 * G + f + p)),
            pl.BlockSpec((QT, BW), lambda p, t, *_: (t, f + p)),
            pl.BlockSpec((QT, BW), lambda p, t, *_: (t, f + p)),
            pl.BlockSpec((HB, S, QT), lambda p, t, *_: (f + p, 0, t)),
            pl.BlockSpec((S, S), lambda p, t, *_: (0, 0)),
        ],
        out_specs=[
            pl.BlockSpec((QT, BW), lambda p, t, *_: (t, p)),
            pl.BlockSpec((S, BW), lambda p, t, *_: (0, p)),
            pl.BlockSpec((S, BW), lambda p, t, *_: (0, p)),
            pl.BlockSpec((CLASSES, HB, 8, LANES), lambda p, t, *_: (0, p, 0, 0)),
        ],
        scratch_shapes=[
            pltpu.VMEM((BW, S), jnp.bfloat16),
            pltpu.VMEM((S, BW), jnp.float32),
            pltpu.VMEM((S, BW), jnp.float32),
            pltpu.VMEM((BW, QT), jnp.float32),
            pltpu.VMEM((HB, 8, QT), jnp.float32),
            pltpu.VMEM((HB, KC, QT), jnp.float32),
        ],
    )
    return pl.pallas_call(
        bwd_kernel,
        grid_spec=gs,
        out_shape=[
            jax.ShapeDtypeStruct((S, W), jnp.bfloat16),
            jax.ShapeDtypeStruct((S, W), jnp.bfloat16),
            jax.ShapeDtypeStruct((S, W), jnp.bfloat16),
            jax.ShapeDtypeStruct((CLASSES, HB * count, 8, LANES), jnp.float32),
        ],
        cost_estimate=pl.CostEstimate(flops=25_000_000_000 * count, bytes_accessed=20_000_000 * count, transcendentals=0),
        name="attn_bwd",
    )(act, lo, hi, qkv, qkv, qkv, d_ctx, ctx32, probs, idx_t)


def block_tables(idx_t):
    S = idx_t.shape[0]
    a = idx_t.reshape(S // SK, SK, S // LANES, LANES)
    real = a < CLASSES
    lo = jnp.min(jnp.where(real, a, CLASSES - 1), axis=(1, 3))
    hi = jnp.max(jnp.where(real, a, 0), axis=(1, 3))
    return lo, hi, jnp.min(a, axis=(1, 3)), jnp.max(a, axis=(1, 3))


def mlp_kernel(rel_ref, u_ref, go_ref, wi0_ref, wi1_ref, wf_ref, z_ref, zrel_ref, dg_ref, du_ref):
    gate = lax.dot_general(u_ref[...], wi0_ref[...], NN, preferred_element_type=jnp.float32)
    up = lax.dot_general(u_ref[...], wi1_ref[...], NN, preferred_element_type=jnp.float32)
    d_act = lax.dot_general(go_ref[...], wf_ref[...], NT, preferred_element_type=jnp.float32).astype(jnp.bfloat16).astype(jnp.float32)
    sig = jax.nn.sigmoid(gate)
    act = gate * sig
    z = (act * up).astype(jnp.bfloat16)
    z_ref[...] = z
    zrel_ref[...] = z
    du_ref[...] = (d_act * act).astype(jnp.bfloat16)
    dg_ref[...] = (d_act * up * (sig * (1.0 + gate * (1.0 - sig)))).astype(jnp.bfloat16)


def mlp_tiles(mlp_in, grad_out, w_i0, w_i1, w_f, rel):
    S, D = mlp_in.shape
    F = w_f.shape[0]
    col = pl.BlockSpec((D, FT), lambda j, r: (0, r[j]))
    out = pl.BlockSpec((S, FT), lambda j, r: (0, r[j]))
    whole = pl.BlockSpec((S, D), lambda j, r: (0, 0))
    gs = pltpu.PrefetchScalarGridSpec(
        num_scalar_prefetch=1,
        grid=(F // FT,),
        in_specs=[whole, whole, col, col, pl.BlockSpec((FT, D), lambda j, r: (r[j], 0))],
        out_specs=[out, pl.BlockSpec((S, FT), lambda j, r: (0, j)), out, out],
    )
    return pl.pallas_call(
        mlp_kernel,
        grid_spec=gs,
        out_shape=[jax.ShapeDtypeStruct((S, F), jnp.bfloat16)] * 4,
        cost_estimate=pl.CostEstimate(flops=12_000_000_000, bytes_accessed=24_000_000, transcendentals=0),
        name="mlp_tiles",
    )(rel, mlp_in, grad_out, w_i0, w_i1, w_f)


def swap(values, axis):
    bit = AXIS_BIT[axis]
    return lax.ppermute(values, ROW_AXES, [(i, i ^ bit) for i in range(16)])


def relative_index(order):
    place = np.arange(16)
    shard_mask = np.zeros(16, np.int32)
    half_mask = np.zeros(16, np.int32)
    for level, axis in enumerate(order):
        bit = (place >> (3 - level)) & 1
        if axis == 'z':
            half_mask += bit
        else:
            shard_mask += bit * AXIS_BIT[axis]
    shard = lax.axis_index('fsdp') ^ jnp.asarray(shard_mask)
    half = lax.axis_index('dp') ^ jnp.asarray(half_mask)
    return shard * 2 + half


def relative_rows(left_t, order):
    depth = left_t.shape[0]
    blocks = left_t.reshape(16, depth // 16, left_t.shape[1])
    return jnp.take(blocks, relative_index(order), axis=0, mode='clip').reshape(left_t.shape)


def product(left_t, right):
    return lax.dot_general(left_t, right, NN, preferred_element_type=jnp.float32)


def product_t(left, right):
    return lax.dot_general(left, right, (((0,), (0,)), ((), ())), preferred_element_type=jnp.float32)


def split(total):
    cut = total.shape[0] // 2
    return total[:cut], total[cut:]


def open_sum(rows, right):
    low, high = split(rows)
    return product(low, right), product(high, right)


def fold(keep, send, axis):
    return split(keep + swap(send, axis))


def close_sum(total):
    mine = total.astype(jnp.bfloat16)
    theirs = swap(mine, 'z')
    first = lax.axis_index('dp') == 0
    return jnp.concatenate([jnp.where(first, mine, theirs), jnp.where(first, theirs, mine)], axis=0)


def together(*values):
    return lax.optimization_barrier(values)


def all_sum(values):
    for axis in 'cxyz':
        values = values + swap(values, axis)
    return values


def gather_full(part):
    return lax.all_gather(part, 'fsdp', axis=0, tiled=True)


def project(tokens_in, weight):
    return lax.dot_general(tokens_in, weight, NN, preferred_element_type=jnp.float32)


def project_t(tokens_in, weight):
    return lax.dot_general(tokens_in, weight, NT, preferred_element_type=jnp.float32)


def rms_norm(values, gain):
    inv_rms = lax.rsqrt(jnp.mean(values * values, axis=-1, keepdims=True) + EPSILON)
    return (values * inv_rms * gain).astype(jnp.bfloat16)


def active_blocks(segments, qkv, rel_bias):
    S = segments.shape[0]
    seg = segments.reshape(S // KC, KC)
    first, last = seg[:, 0], seg[:, -1]
    meet = (first[:, None] <= last[None, :]) & (last[:, None] >= first[None, :])
    width = rel_bias.shape[1] * HD
    reach = HD * jnp.max(jnp.abs(qkv[:, :width])).astype(jnp.float32) * jnp.max(jnp.abs(qkv[:, width:2 * width])).astype(jnp.float32)
    bound = 2.0 * reach + 2.0 * jnp.max(jnp.abs(rel_bias))
    safe = bound < 0.9e9
    return (meet | ~safe).astype(jnp.int32)


def local_layer(x_in, positions, segments, rel_bias, gain_attn, gain_mlp, wq_part, wk_part, wv_part, wo_part, wi0_part, wi1_part, wf_part, grad_out):
    S, D = x_in.shape[1], x_in.shape[2]
    heads = rel_bias.shape[1]
    x_float = x_in[0].astype(jnp.float32)
    positions, segments, grad_out = positions[0], segments[0], grad_out[0]
    w_qkv = gather_full(jnp.concatenate([wq_part, wk_part, wv_part], axis=1))
    w_o = gather_full(wo_part)
    w_i0 = gather_full(wi0_part)
    w_i1 = gather_full(wi1_part)
    w_f = gather_full(wf_part)

    idx_t = class_index(positions[None, :], positions[:, None], segments[None, :], segments[:, None])
    lo, hi, lo_all, hi_all = block_tables(idx_t)
    tab = bias_table(rel_bias)

    normed, norm1_pull = jax.vjp(lambda gain: rms_norm(x_float, gain), gain_attn)
    qkv = project(normed, w_qkv).astype(jnp.bfloat16)
    act = active_blocks(segments, qkv, rel_bias)
    context, ctx32, probs = attn_fwd(qkv, idx_t, tab, tab[:, 0, :2 * CLASSES], act, lo_all, hi_all)
    hidden = (x_float + project(context, w_o)).astype(jnp.bfloat16)
    h_float = hidden.astype(jnp.float32)
    mlp_in, norm2_pull = jax.vjp(rms_norm, h_float, gain_mlp)
    hidden_act, act_rel, d_gate, d_up = mlp_tiles(mlp_in, grad_out, w_i0, w_i1, w_f, relative_index('cxyz')[::2] // 2)

    ow, oi0, oi1 = 'cxyz', 'cyzx', 'czxy'
    half = act_rel.shape[1] // 2
    mlp_in_t = mlp_in.T
    kw, sw = product_t(act_rel[:, :half], grad_out), product_t(act_rel[:, half:], grad_out)
    k0, s0 = open_sum(relative_rows(mlp_in_t, oi0), d_gate)
    k1, s1 = open_sum(relative_rows(mlp_in_t, oi1), d_up)
    kw, sw = fold(kw, sw, ow[0])
    k0, s0 = fold(k0, s0, oi0[0])
    k1, s1 = fold(k1, s1, oi1[0])
    d_mlp_in = (project_t(d_gate, w_i0) + project_t(d_up, w_i1)).astype(jnp.bfloat16)
    d_h_norm, d_gain_mlp = norm2_pull(d_mlp_in)
    d_hidden = (grad_out.astype(jnp.float32) + d_h_norm).astype(jnp.bfloat16)
    oo = 'cxyz'
    ko, so = open_sum(relative_rows(context.T, oo), d_hidden)
    y_out = (h_float + project(hidden_act, w_f)).astype(jnp.bfloat16)
    d_context = project_t(d_hidden, w_o).astype(jnp.bfloat16)

    parts = []
    d_context, sw, s0, s1, so, y_out = together(d_context, sw, s0, s1, so, y_out)
    parts.append(attn_bwd(qkv, d_context, ctx32, probs, idx_t, act, lo, hi, 0, 1))
    kw, sw = fold(kw, sw, ow[1])
    k0, s0 = fold(k0, s0, oi0[1])
    k1, s1 = fold(k1, s1, oi1[1])
    ko, so = fold(ko, so, oo[0])
    d_context, sw, s0, s1, so, head = together(d_context, sw, s0, s1, so, parts[0])
    parts[0] = head
    parts.append(attn_bwd(qkv, d_context, ctx32, probs, idx_t, act, lo, hi, 1, 1))
    first_half, second_half = fold(kw, sw, ow[2])
    near = lax.axis_index('dp') == 0
    kw, sw = jnp.where(near, first_half, second_half), jnp.where(near, second_half, first_half)
    k0, s0 = fold(k0, s0, oi0[2])
    k1, s1 = fold(k1, s1, oi1[2])
    ko, so = fold(ko, so, oo[1])
    d_context, sw, s0, s1, so, head = together(d_context, sw, s0, s1, so, parts[1])
    parts[1] = head
    parts.append(attn_bwd(qkv, d_context, ctx32, probs, idx_t, act, lo, hi, 2, 1))
    gw = kw + swap(sw, 'z')
    g0 = k0 + swap(s0, oi0[3])
    g1 = k1 + swap(s1, oi1[3])
    ko, so = fold(ko, so, oo[2])
    gw, g0, g1, so, head = together(gw, g0, g1, so, parts[2])
    parts[2] = head
    go = ko + swap(so, oo[3])
    d_wf, d_wi0, d_wi1, d_wo = close_sum(gw), close_sum(g0), close_sum(g1), close_sum(go)

    d_q, d_k, d_v = [jnp.concatenate([part[n] for part in parts], axis=1) for n in range(3)]
    d_bias = jnp.concatenate([jnp.sum(part[3], axis=(2, 3)) for part in parts], axis=1)
    normed_t = normed.T
    last = []
    for value, order in ((d_q, 'cxyz'), (d_k, 'cyzx'), (d_v, 'czxy')):
        keep, send = open_sum(relative_rows(normed_t, order), value)
        for axis in order[:3]:
            keep, send = fold(keep, send, axis)
        last.append(close_sum(keep + swap(send, order[3])))
    d_wq, d_wk, d_wv = last
    d_normed = project_t(jnp.concatenate([d_q, d_k, d_v], axis=1), w_qkv).astype(jnp.bfloat16)
    d_gain_attn = norm1_pull(d_normed)[0]
    small = jnp.concatenate([d_bias.reshape(-1), d_gain_attn, d_gain_mlp])
    small = all_sum(jnp.pad(small, (0, 2048 - small.shape[0])).reshape(16, 128)).reshape(-1)
    n_bias = CLASSES * heads
    return (y_out[None], small[:n_bias].reshape(CLASSES, heads), small[n_bias:n_bias + D], small[n_bias + D:n_bias + 2 * D],
            d_wq, d_wk, d_wv, d_wo, d_wi0, d_wi1, d_wf)


def solution(mesh):
    row_spec = P(ROW_AXES)
    whole = P()
    part_spec = P('fsdp')
    in_specs = (row_spec, row_spec, row_spec, whole, whole, whole) + (part_spec,) * 7 + (row_spec,)
    out_specs = (row_spec, whole, whole, whole) + (part_spec,) * 7
    return jax.shard_map(local_layer, mesh=mesh, in_specs=in_specs, out_specs=out_specs, check_vma=False)
```

```python
import jax
import jax.numpy as jnp
import numpy as np
from jax import lax
from jax.experimental import pallas as pl
from jax.experimental.pallas import tpu as pltpu
from jax.sharding import PartitionSpec as P

EPSILON = 1e-6
NEG_BIG = -1e9
CLASSES = 32
HALF_CLASSES = 16
EXACT_RANGE = 8
THRESHOLDS = (12, 16, 23, 32, 46, 64, 91)
ROW_AXES = ('dp', 'fsdp')
LANES = 128
QT = 256
KC = 256
SK = 64
HB = 4
HD = 64
NKS = KC // SK
NQS = QT // LANES
FT = 256

NT = (((1,), (1,)), ((), ()))
NN = (((1,), (0,)), ((), ()))
AXIS_BIT = {'c': 1, 'x': 2, 'y': 4, 'z': 8}


def class_index(pos_q, pos_k, seg_q, seg_k):
    offset = pos_k - pos_q
    distance = jnp.abs(offset)
    magnitude = jnp.minimum(distance, EXACT_RANGE)
    for bound in THRESHOLDS:
        magnitude = magnitude + (distance >= bound).astype(jnp.int32)
    rel_cls = magnitude + HALF_CLASSES * (offset > 0).astype(jnp.int32)
    return rel_cls + CLASSES * (seg_q != seg_k).astype(jnp.int32)


def bias_table(rel_bias):
    both = jnp.concatenate([rel_bias, rel_bias + NEG_BIG], axis=0).T
    heads = both.shape[0]
    tab = jnp.pad(both, ((0, 0), (0, LANES - 2 * CLASSES)))
    return jnp.broadcast_to(tab[:, None, :], (heads, 8, LANES))


def lookup(tab, idx):
    rows, cols = idx.shape
    tab_rows = jnp.concatenate([tab] * (rows // 8), axis=0) if rows > 8 else tab
    parts = []
    for j in range(cols // LANES):
        parts.append(jnp.take_along_axis(tab_rows, idx[:, j * LANES:(j + 1) * LANES], axis=1, mode='promise_in_bounds'))
    return jnp.concatenate(parts, axis=1)


def head_lanes(x, h):
    lane = lax.broadcasted_iota(jnp.int32, x.shape, 1)
    return jnp.where((lane >= HD * h) & (lane < HD * (h + 1)), x, jnp.zeros_like(x))


def fwd_kernel(mode_ref, only_ref, tabs_ref, q_ref, k_ref, v_ref, idx_ref, tab_ref,
               ctx_ref, ctx32_ref, p_ref, vt_scr, m_scr, l_scr, o_scr):
    g = pl.program_id(0)
    t = pl.program_id(1)
    S = k_ref.shape[0]

    @pl.when(t == 0)
    def _():
        for j in range(HB // 2):
            vt_scr[j * LANES:(j + 1) * LANES, :] = v_ref[:, j * LANES:(j + 1) * LANES].astype(jnp.float32).T.astype(jnp.bfloat16)

    m_scr[...] = jnp.full(m_scr.shape, -jnp.inf, jnp.float32)
    l_scr[...] = jnp.zeros_like(l_scr)
    o_scr[...] = jnp.zeros_like(o_scr)

    def scores(c, h):
        js = slice((h // 2) * LANES, (h // 2 + 1) * LANES)
        ks = slice(c * KC, (c + 1) * KC)
        return lax.dot_general(head_lanes(k_ref[ks, js], h % 2), q_ref[:, js], NT, preferred_element_type=jnp.float32)

    for c in range(S // KC):
        ks = slice(c * KC, (c + 1) * KC)

        @pl.when(mode_ref[c, t] == 1)
        def _(c=c, ks=ks):
            for h in range(HB):
                s = scores(c, h) + tabs_ref[g * HB + h, only_ref[c, t]]
                p_ref[h, ks, :] = s
                m_scr[h] = jnp.maximum(m_scr[h], jnp.max(s.reshape(KC // 8, 8, QT), axis=0))

        @pl.when(mode_ref[c, t] == 2)
        def _(c=c, ks=ks):
            idx = idx_ref[ks, pl.ds(pl.multiple_of(t * QT, QT), QT)]
            for h in range(HB):
                s = scores(c, h) + lookup(tab_ref[h], idx)
                p_ref[h, ks, :] = s
                m_scr[h] = jnp.maximum(m_scr[h], jnp.max(s.reshape(KC // 8, 8, QT), axis=0))

    for h in range(HB):
        m_scr[h] = jnp.broadcast_to(jnp.max(m_scr[h], axis=0, keepdims=True), (8, QT))
    for c in range(S // KC):
        @pl.when(mode_ref[c, t] != 0)
        def _(c=c):
            ks = slice(c * KC, (c + 1) * KC)
            for h in range(HB):
                e = jnp.exp(p_ref[h, ks, :].reshape(KC // 8, 8, QT) - m_scr[h])
                p_ref[h, ks, :] = e.reshape(KC, QT)
                l_scr[h] += jnp.sum(e, axis=0)
    for h in range(HB):
        l_scr[h] = jnp.broadcast_to(1.0 / jnp.sum(l_scr[h], axis=0, keepdims=True), (8, QT))
    for c in range(S // KC):
        @pl.when(mode_ref[c, t] != 0)
        def _(c=c):
            ks = slice(c * KC, (c + 1) * KC)
            for h in range(HB):
                pr = (p_ref[h, ks, :].reshape(KC // 8, 8, QT) * l_scr[h]).reshape(KC, QT)
                p_ref[h, ks, :] = pr
                hs = slice(h * HD, (h + 1) * HD)
                o_scr[hs, :] += lax.dot_general(vt_scr[hs, ks], pr.astype(jnp.bfloat16), NN, preferred_element_type=jnp.float32)
    o = o_scr[...].T
    ctx32_ref[...] = o
    ctx_ref[...] = o.astype(jnp.bfloat16)


def attn_fwd(qkv, idx_t, tab, tabs, mode, only):
    S = qkv.shape[0]
    heads = tab.shape[0]
    G = heads // HB
    BW = HB * HD
    W = heads * HD
    gs = pltpu.PrefetchScalarGridSpec(
        num_scalar_prefetch=3,
        grid=(G, S // QT),
        in_specs=[
            pl.BlockSpec((QT, BW), lambda p, t, *_: (t, p)),
            pl.BlockSpec((S, BW), lambda p, t, *_: (0, G + p)),
            pl.BlockSpec((S, BW), lambda p, t, *_: (0, 2 * G + p)),
            pl.BlockSpec((S, S), lambda p, t, *_: (0, 0)),
            pl.BlockSpec((HB, 8, LANES), lambda p, t, *_: (p, 0, 0)),
        ],
        out_specs=[
            pl.BlockSpec((QT, BW), lambda p, t, *_: (t, p)),
            pl.BlockSpec((QT, BW), lambda p, t, *_: (t, p)),
            pl.BlockSpec((HB, S, QT), lambda p, t, *_: (p, 0, t)),
        ],
        scratch_shapes=[pltpu.VMEM((BW, S), jnp.bfloat16), pltpu.VMEM((HB, 8, QT), jnp.float32),
                        pltpu.VMEM((HB, 8, QT), jnp.float32), pltpu.VMEM((BW, QT), jnp.float32)],
    )
    return pl.pallas_call(
        fwd_kernel,
        grid_spec=gs,
        out_shape=[
            jax.ShapeDtypeStruct((S, W), jnp.bfloat16),
            jax.ShapeDtypeStruct((S, W), jnp.float32),
            jax.ShapeDtypeStruct((heads, S, S), jnp.float32),
        ],
        cost_estimate=pl.CostEstimate(flops=40_000_000_000, bytes_accessed=60_000_000, transcendentals=0),
        name="attn_fwd",
    )(mode, only, tabs, qkv, qkv, qkv, idx_t, tab)


def bwd_kernel(act_ref, cls_ref, q_ref, k_ref, v_ref, dc_ref, ctx32_ref, p_ref, posk_ref, posq_ref, eq_ref, ekt_ref,
               dq_ref, dk_ref, dv_ref, dr_ref, db_ref, kt_scr, dk_acc, dv_acc, dqt_acc, dlt_scr, eq2_scr, x_acc):
    t = pl.program_id(1)
    S = k_ref.shape[0]

    @pl.when(t == 0)
    def _():
        for j in range(HB // 2):
            js = slice(j * LANES, (j + 1) * LANES)
            kt_scr[js, :] = k_ref[:, js].astype(jnp.float32).T.astype(jnp.bfloat16)
        dk_acc[...] = jnp.zeros_like(dk_acc)
        dv_acc[...] = jnp.zeros_like(dv_acc)
        db_ref[...] = jnp.zeros_like(db_ref)
        dr_ref[...] = jnp.zeros_like(dr_ref)
        x_acc[...] = jnp.zeros_like(x_acc)

    eq2_scr[:QT, :] = eq_ref[...]
    eq2_scr[QT:, :] = eq_ref[...]
    dqt_acc[...] = jnp.zeros_like(dqt_acc)
    for j in range(HB // 2):
        js = slice(j * LANES, (j + 1) * LANES)
        prod_t = (ctx32_ref[:, js] * dc_ref[:, js].astype(jnp.float32)).T
        for h in range(2):
            d = jnp.sum(prod_t[HD * h:HD * (h + 1), :], axis=0, keepdims=True)
            dlt_scr[2 * j + h] = jnp.broadcast_to(d, (8, QT))

    def chunk(c, finish):
        ks = slice(c * KC, (c + 1) * KC)
        for h in range(HB):
            js = slice((h // 2) * LANES, (h // 2 + 1) * LANES)
            hs = slice(h * HD, (h + 1) * HD)
            dp = lax.dot_general(head_lanes(v_ref[ks, js], h % 2), dc_ref[:, js], NT, preferred_element_type=jnp.float32)
            pr = p_ref[h, ks, :]
            ds = pr * (dp.reshape(KC // 8, 8, QT) - dlt_scr[h]).reshape(KC, QT)
            ds16 = ds.astype(jnp.bfloat16)
            dv_acc[ks, js] += lax.dot_general(pr.astype(jnp.bfloat16), head_lanes(dc_ref[:, js], h % 2), NN, preferred_element_type=jnp.float32)
            dk_acc[ks, js] += lax.dot_general(ds16, head_lanes(q_ref[:, js], h % 2), NN, preferred_element_type=jnp.float32)
            dqt_acc[hs, :] += lax.dot_general(kt_scr[hs, ks], ds16, NN, preferred_element_type=jnp.float32)
            finish(h, ks, ds)

    for c in range(S // KC):
        @pl.when(act_ref[c, t] == 1)
        def _(c=c):
            only = cls_ref[c, t]

            def finish(h, ks, ds):
                part = jnp.sum(ds.reshape(KC // 8, 8, QT), axis=0)
                db_ref[only, h] += part[:, :LANES] + part[:, LANES:]

            chunk(c, finish)

        @pl.when(act_ref[c, t] == 2)
        def _(c=c):
            pk = posk_ref[c * KC:(c + 1) * KC, :]
            offset = jnp.concatenate([pk, pk], axis=1) - posq_ref[0:1, :]
            above = offset >= THRESHOLDS[-1]
            far = jnp.abs(offset) >= THRESHOLDS[-1]

            def finish(h, ks, ds):
                near = jnp.where(far, 0.0, ds)
                hi16 = near.astype(jnp.bfloat16)
                lo16 = (near - hi16.astype(jnp.float32)).astype(jnp.bfloat16)
                x_acc[h, ks, :] += lax.dot_general(jnp.concatenate([hi16, lo16], axis=1), eq2_scr[...], NN, preferred_element_type=jnp.float32)
                up = jnp.sum(jnp.where(above, ds, 0.0).reshape(KC // 8, 8, QT), axis=0)
                out = jnp.sum(jnp.where(far, ds, 0.0).reshape(KC // 8, 8, QT), axis=0) - up
                db_ref[CLASSES - 1, h] += up[:, :LANES] + up[:, LANES:]
                db_ref[HALF_CLASSES - 1, h] += out[:, :LANES] + out[:, LANES:]

            chunk(c, finish)

    dq_ref[...] = dqt_acc[...].T.astype(jnp.bfloat16)

    @pl.when(t == pl.num_programs(1) - 1)
    def _():
        dk_ref[...] = dk_acc[...].astype(jnp.bfloat16)
        dv_ref[...] = dv_acc[...].astype(jnp.bfloat16)
        for h in range(HB):
            x = x_acc[h]
            hi16 = x.astype(jnp.bfloat16)
            lo16 = (x - hi16.astype(jnp.float32)).astype(jnp.bfloat16)
            pairs = (lax.dot_general(ekt_ref[...], hi16, NN, preferred_element_type=jnp.float32)
                     + lax.dot_general(ekt_ref[...], lo16, NN, preferred_element_type=jnp.float32))
            turned = pltpu.roll(pairs, 0, 1, stride=1, stride_axis=0)
            by_class = jnp.sum(db_ref[:, h].reshape(CLASSES, 8, LANES), axis=1)
            whole = jnp.sum(by_class, axis=1, keepdims=True)
            cls = lax.broadcasted_iota(jnp.int32, (CLASSES, 256), 0)
            lane = lax.broadcasted_iota(jnp.int32, (CLASSES, 256), 1)
            home = jnp.where(cls == CLASSES - 1, 100, jnp.where(cls == HALF_CLASSES - 1, 156, -1))
            dr_ref[0, h:h + 1, :] = jnp.sum(turned, axis=0, keepdims=True) + jnp.sum(jnp.where(lane == home, whole, 0.0), axis=0, keepdims=True)


def attn_bwd(qkv, d_ctx, ctx32, probs, posk, posq, act, cls, eq, ekt, first, count):
    S = qkv.shape[0]
    heads = probs.shape[0]
    G = heads // HB
    BW = HB * HD
    W = count * BW
    f = first
    gs = pltpu.PrefetchScalarGridSpec(
        num_scalar_prefetch=2,
        grid=(count, S // QT),
        in_specs=[
            pl.BlockSpec((QT, BW), lambda p, t, *_: (t, f + p)),
            pl.BlockSpec((S, BW), lambda p, t, *_: (0, G + f + p)),
            pl.BlockSpec((S, BW), lambda p, t, *_: (0, 2 * G + f + p)),
            pl.BlockSpec((QT, BW), lambda p, t, *_: (t, f + p)),
            pl.BlockSpec((QT, BW), lambda p, t, *_: (t, f + p)),
            pl.BlockSpec((HB, S, QT), lambda p, t, *_: (f + p, 0, t)),
            pl.BlockSpec((S, LANES), lambda p, t, *_: (0, 0)),
            pl.BlockSpec((8, QT), lambda p, t, *_: (0, t)),
            pl.BlockSpec((QT, 256), lambda p, t, *_: (t, 0)),
            pl.BlockSpec((256, S), lambda p, t, *_: (0, 0)),
        ],
        out_specs=[
            pl.BlockSpec((QT, BW), lambda p, t, *_: (t, p)),
            pl.BlockSpec((S, BW), lambda p, t, *_: (0, p)),
            pl.BlockSpec((S, BW), lambda p, t, *_: (0, p)),
            pl.BlockSpec((1, 8, 256), lambda p, t, *_: (p, 0, 0)),
        ],
        scratch_shapes=[
            pltpu.VMEM((CLASSES, HB, 8, LANES), jnp.float32),
            pltpu.VMEM((BW, S), jnp.bfloat16),
            pltpu.VMEM((S, BW), jnp.float32),
            pltpu.VMEM((S, BW), jnp.float32),
            pltpu.VMEM((BW, QT), jnp.float32),
            pltpu.VMEM((HB, 8, QT), jnp.float32),
            pltpu.VMEM((2 * QT, 256), jnp.bfloat16),
            pltpu.VMEM((HB, S, 256), jnp.float32),
        ],
    )
    return pl.pallas_call(
        bwd_kernel,
        grid_spec=gs,
        out_shape=[
            jax.ShapeDtypeStruct((S, W), jnp.bfloat16),
            jax.ShapeDtypeStruct((S, W), jnp.bfloat16),
            jax.ShapeDtypeStruct((S, W), jnp.bfloat16),
            jax.ShapeDtypeStruct((count, 8, 256), jnp.float32),
        ],
        cost_estimate=pl.CostEstimate(flops=25_000_000_000 * count, bytes_accessed=20_000_000 * count, transcendentals=0),
        name="attn_bwd",
    )(act, cls, qkv, qkv, qkv, d_ctx, ctx32, probs, posk, posq, eq, ekt)


def spread(positions):
    S = positions.shape[0]
    return jnp.broadcast_to(positions[:, None], (S, LANES)), jnp.broadcast_to(positions[None, :], (8, S))


def place_onehots(positions):
    lane = jnp.arange(256, dtype=jnp.int32)
    eq = ((-positions[:, None]) & 255) == lane[None, :]
    ekt = (positions[None, :] & 255) == lane[:, None]
    return eq.astype(jnp.bfloat16), ekt.astype(jnp.bfloat16)


def mlp_kernel(rel_ref, u_ref, go_ref, wi0_ref, wi1_ref, wf_ref, z_ref, zrel_ref, dg_ref, du_ref):
    gate = lax.dot_general(u_ref[...], wi0_ref[...], NN, preferred_element_type=jnp.float32)
    up = lax.dot_general(u_ref[...], wi1_ref[...], NN, preferred_element_type=jnp.float32)
    d_act = lax.dot_general(go_ref[...], wf_ref[...], NT, preferred_element_type=jnp.float32).astype(jnp.bfloat16).astype(jnp.float32)
    sig = jax.nn.sigmoid(gate)
    act = gate * sig
    z = (act * up).astype(jnp.bfloat16)
    z_ref[...] = z
    zrel_ref[...] = z
    du_ref[...] = (d_act * act).astype(jnp.bfloat16)
    dg_ref[...] = (d_act * up * (sig * (1.0 + gate * (1.0 - sig)))).astype(jnp.bfloat16)


def mlp_tiles(mlp_in, grad_out, w_i0, w_i1, w_f, rel):
    S, D = mlp_in.shape
    F = w_f.shape[0]
    col = pl.BlockSpec((D, FT), lambda j, r: (0, r[j]))
    out = pl.BlockSpec((S, FT), lambda j, r: (0, r[j]))
    whole = pl.BlockSpec((S, D), lambda j, r: (0, 0))
    gs = pltpu.PrefetchScalarGridSpec(
        num_scalar_prefetch=1,
        grid=(F // FT,),
        in_specs=[whole, whole, col, col, pl.BlockSpec((FT, D), lambda j, r: (r[j], 0))],
        out_specs=[out, pl.BlockSpec((S, FT), lambda j, r: (0, j)), out, out],
    )
    return pl.pallas_call(
        mlp_kernel,
        grid_spec=gs,
        out_shape=[jax.ShapeDtypeStruct((S, F), jnp.bfloat16)] * 4,
        cost_estimate=pl.CostEstimate(flops=12_000_000_000, bytes_accessed=24_000_000, transcendentals=0),
        name="mlp_tiles",
    )(rel, mlp_in, grad_out, w_i0, w_i1, w_f)


def swap(values, axis):
    bit = AXIS_BIT[axis]
    return lax.ppermute(values, ROW_AXES, [(i, i ^ bit) for i in range(16)])


def relative_index(order):
    place = np.arange(16)
    shard_mask = np.zeros(16, np.int32)
    half_mask = np.zeros(16, np.int32)
    for level, axis in enumerate(order):
        bit = (place >> (3 - level)) & 1
        if axis == 'z':
            half_mask += bit
        else:
            shard_mask += bit * AXIS_BIT[axis]
    shard = lax.axis_index('fsdp') ^ jnp.asarray(shard_mask)
    half = lax.axis_index('dp') ^ jnp.asarray(half_mask)
    return shard * 2 + half


def relative_rows(left_t, order):
    depth = left_t.shape[0]
    blocks = left_t.reshape(16, depth // 16, left_t.shape[1])
    return jnp.take(blocks, relative_index(order), axis=0, mode='clip').reshape(left_t.shape)


def product(left_t, right):
    return lax.dot_general(left_t, right, NN, preferred_element_type=jnp.float32)


def product_t(left, right):
    return lax.dot_general(left, right, (((0,), (0,)), ((), ())), preferred_element_type=jnp.float32)


def split(total):
    cut = total.shape[0] // 2
    return total[:cut], total[cut:]


def open_sum(rows, right):
    low, high = split(rows)
    return product(low, right), product(high, right)


def fold(keep, send, axis):
    return split(keep + swap(send, axis))


def close_sum(total):
    mine = total.astype(jnp.bfloat16)
    theirs = swap(mine, 'z')
    first = lax.axis_index('dp') == 0
    return jnp.concatenate([jnp.where(first, mine, theirs), jnp.where(first, theirs, mine)], axis=0)


def together(*values):
    return lax.optimization_barrier(values)


TAIL_ORDERS = ('xyz', 'yxz', 'zxy')
TAIL_DIM = {'y': 0, 'x': 1, 'z': 2}


def partner_id(axis):
    z, f = lax.axis_index('dp'), lax.axis_index('fsdp')
    return (z ^ 1, f) if axis == 'z' else (z, f ^ AXIS_BIT[axis])


def remote(src, dst, sems, n, axis):
    return pltpu.make_async_remote_copy(src_ref=src, dst_ref=dst, send_sem=sems.at[0, n], recv_sem=sems.at[1, n],
                                        device_id=partner_id(axis), device_id_type=pl.DeviceIdType.MESH)


def tail_index(order, level, bit):
    index = [slice(None)] * 3
    for n in range(level):
        index[TAIL_DIM[order[n]]] = 0
    index[TAIL_DIM[order[level]]] = bit
    return tuple(index)


def tail_kernel(*refs):
    n_groups = 3
    nt_ref, x_ref, w_ref = refs[:3]
    grads = [refs[3 + 3 * p:6 + 3 * p] for p in range(3)]
    dbias_refs = refs[12:15]
    gmlp_ref = refs[15]
    extra_in = refs[16:19]
    out_refs = refs[19:22]
    extra_out = refs[22:25]
    small_out = refs[25]
    lhs_send, lhs_keep, snd, rcv_c, acc, rcv1, rcv2, rcv3, small, small_rcv, mine, dn_acc, sems = refs[26:]
    z, f = lax.axis_index('dp'), lax.axis_index('fsdp')
    rows = nt_ref.shape[0] // 16
    BW = grads[0][0].shape[1]

    barrier = pltpu.get_barrier_semaphore()
    for axis in 'cxyz':
        pl.semaphore_signal(barrier, inc=1, device_id=partner_id(axis), device_id_type=pl.DeviceIdType.MESH)
    pl.semaphore_wait(barrier, 4)

    extra = []
    for n in range(3):
        extra_out[n][z] = extra_in[n][...]
        copy = remote(extra_in[n], extra_out[n].at[z], sems, n, 'z')
        copy.start()
        extra.append(copy)

    for by in range(2):
        for bx in range(2):
            for bh in range(2):
                place = slice(((by * 2 + bx) * 2 + bh) * rows, ((by * 2 + bx) * 2 + bh + 1) * rows)
                shard = f ^ (4 * by + 2 * bx)
                for core, lhs in ((1, lhs_send), (0, lhs_keep)):
                    start = pl.multiple_of(((shard ^ core) * 2 + (z ^ bh)) * rows, 16)
                    lhs[place, :] = nt_ref[pl.ds(start, rows), :]

    core_copies = []
    for p in range(3):
        for g in range(n_groups):
            cols = slice(g * BW, (g + 1) * BW)
            snd[p, :, cols] = lax.dot_general(lhs_send[...], grads[p][g][...], NN, preferred_element_type=jnp.float32)
        copy = remote(snd.at[p], rcv_c.at[p], sems, 3 + p, 'c')
        copy.start()
        core_copies.append(copy)

    first = []
    for p in range(3):
        for g in range(n_groups):
            cols = slice(g * BW, (g + 1) * BW)
            own = lax.dot_general(lhs_keep[...], grads[p][g][...], NN, preferred_element_type=jnp.float32)
            acc[p, :, :, :, :, cols] = own.reshape(2, 2, 2, rows, BW)
        core_copies[p].wait()
        acc[p] += rcv_c[p].reshape(2, 2, 2, rows, n_groups * BW)
        order = TAIL_ORDERS[p]
        copy = remote(acc.at[(p,) + tail_index(order, 0, 1)], rcv1.at[p], sems, 6 + p, order[0])
        copy.start()
        first.append(copy)

    S = x_ref.shape[0]
    dn_acc[...] = jnp.zeros_like(dn_acc)

    @pl.loop(0, S // 256)
    def _(i):
        tok = pl.ds(pl.multiple_of(i * 256, 256), 256)
        d_normed = None
        for p in range(3):
            for g in range(n_groups):
                cols = slice((p * n_groups + g) * BW, (p * n_groups + g + 1) * BW)
                term = lax.dot_general(grads[p][g][tok, :], w_ref[:, cols], NT, preferred_element_type=jnp.float32)
                d_normed = term if d_normed is None else d_normed + term
        xf = x_ref[tok, :].astype(jnp.float32)
        inv = lax.rsqrt(jnp.mean(xf * xf, axis=1, keepdims=True) + EPSILON)
        term = d_normed.astype(jnp.bfloat16).astype(jnp.float32) * (xf * inv)
        dn_acc[...] += jnp.sum(term.reshape(32, 8, term.shape[1]), axis=0)

    small[0] = jnp.zeros(small.shape[1:], jnp.float32)
    offset = lax.broadcasted_iota(jnp.int32, (256, LANES), 0)
    offset = jnp.where(offset < 128, offset, offset - 256)
    table = (class_index(0, offset, offset, offset) == lax.broadcasted_iota(jnp.int32, (256, LANES), 1)).astype(jnp.float32).astype(jnp.bfloat16)
    by_offset = jnp.concatenate([r[0] for r in dbias_refs], axis=0)
    for _ in range(3):
        piece = by_offset.astype(jnp.bfloat16)
        small[0, 0:8 * n_groups, :] += lax.dot_general(piece, table, NN, preferred_element_type=jnp.float32)
        by_offset = by_offset - piece.astype(jnp.float32)
    small[0, 24:30, :] = gmlp_ref[...]
    d_gain = jnp.sum(dn_acc[...], axis=0, keepdims=True)
    for n in range(6):
        small[0, 32 + n:33 + n, :] = d_gain[:, n * LANES:(n + 1) * LANES]

    def small_copy(n):
        return remote(small.at[n], small_rcv.at[n], sems, 15 + n, 'cxyz'[n])

    small_copy(0).start()

    second = []
    for p in range(3):
        order = TAIL_ORDERS[p]
        first[p].wait()
        acc[(p,) + tail_index(order, 0, 0)] += rcv1[p]
        copy = remote(acc.at[(p,) + tail_index(order, 1, 1)], rcv2.at[p], sems, 9 + p, order[1])
        copy.start()
        second.append(copy)
    small_copy(0).wait()
    small[1] = small[0] + small_rcv[0]
    small_copy(1).start()
    third = []
    for p in range(3):
        order = TAIL_ORDERS[p]
        second[p].wait()
        acc[(p,) + tail_index(order, 1, 0)] += rcv2[p]
        copy = remote(acc.at[(p,) + tail_index(order, 2, 1)], rcv3.at[p], sems, 12 + p, order[2])
        copy.start()
        third.append(copy)
    small_copy(1).wait()
    small[2] = small[1] + small_rcv[1]
    small_copy(2).start()
    last = []
    for p in range(3):
        third[p].wait()
        total = (acc[p, 0, 0, 0] + rcv3[p]).astype(jnp.bfloat16)
        mine[p] = total
        out_refs[p][z] = total
        copy = remote(mine.at[p], out_refs[p].at[z], sems, 19 + p, 'z')
        copy.start()
        last.append(copy)
    small_copy(2).wait()
    small[3] = small[2] + small_rcv[2]
    small_copy(3).start()
    for copy in extra + last:
        copy.wait()
    small_copy(3).wait()
    small_out[...] = small[3] + small_rcv[3]


def tail_reduce(normed_t, x_row, w_qkv, grads, dbias, gain_mlp_rows, extra):
    D, S = normed_t.shape
    rows = D // 16
    W = 3 * grads[0][0].shape[1]
    vm = pl.BlockSpec(memory_space=pltpu.VMEM)
    shapes = [jax.ShapeDtypeStruct((2, rows, W), jnp.bfloat16)] * 3
    shapes += [jax.ShapeDtypeStruct((2,) + e.shape, jnp.bfloat16) for e in extra]
    shapes += [jax.ShapeDtypeStruct((40, LANES), jnp.float32)]
    outs = pl.pallas_call(
        tail_kernel,
        in_specs=[vm] * 19,
        out_specs=[vm] * 7,
        out_shape=shapes,
        scratch_shapes=[
            pltpu.VMEM((D // 2, S), jnp.bfloat16),
            pltpu.VMEM((D // 2, S), jnp.bfloat16),
            pltpu.VMEM((3, D // 2, W), jnp.float32),
            pltpu.VMEM((3, D // 2, W), jnp.float32),
            pltpu.VMEM((3, 2, 2, 2, rows, W), jnp.float32),
            pltpu.VMEM((3, 2, 2, rows, W), jnp.float32),
            pltpu.VMEM((3, 2, rows, W), jnp.float32),
            pltpu.VMEM((3, rows, W), jnp.float32),
            pltpu.VMEM((4, 40, LANES), jnp.float32),
            pltpu.VMEM((4, 40, LANES), jnp.float32),
            pltpu.VMEM((3, rows, W), jnp.bfloat16),
            pltpu.VMEM((8, D), jnp.float32),
            pltpu.SemaphoreType.DMA((2, 22)),
        ],
        compiler_params=pltpu.CompilerParams(collective_id=1, has_side_effects=True),
        cost_estimate=pl.CostEstimate(flops=12_000_000_000, bytes_accessed=14_000_000, transcendentals=0),
        name="tail_reduce",
    )(normed_t, x_row, w_qkv, *[a for part in grads for a in part], *dbias, gain_mlp_rows, *extra)
    full = [o.reshape(2 * o.shape[1], o.shape[2]) for o in outs[:6]]
    return full, outs[6]


def gather_full(part):
    return lax.all_gather(part, 'fsdp', axis=0, tiled=True)


def project(tokens_in, weight):
    return lax.dot_general(tokens_in, weight, NN, preferred_element_type=jnp.float32)


def project_t(tokens_in, weight):
    return lax.dot_general(tokens_in, weight, NT, preferred_element_type=jnp.float32)


def rms_norm(values, gain):
    inv_rms = lax.rsqrt(jnp.mean(values * values, axis=-1, keepdims=True) + EPSILON)
    return (values * inv_rms * gain).astype(jnp.bfloat16)


def block_modes(positions, segments, qkv, rel_bias):
    pos = positions.reshape(-1, KC)
    seg = segments.reshape(-1, KC)
    first, last = seg[:, 0], seg[:, -1]
    meet = (first[:, None] <= last[None, :]) & (last[:, None] >= first[None, :])
    width = rel_bias.shape[1] * HD
    reach = HD * jnp.max(jnp.abs(qkv[:, :width])).astype(jnp.float32) * jnp.max(jnp.abs(qkv[:, width:2 * width])).astype(jnp.float32)
    safe = 2.0 * reach + 2.0 * jnp.max(jnp.abs(rel_bias)) < 0.9e9
    active = meet | ~safe
    least, most = jnp.min(pos, axis=1), jnp.max(pos, axis=1)
    above = least[:, None] - most[None, :] >= THRESHOLDS[-1]
    below = most[:, None] - least[None, :] <= -THRESHOLDS[-1]
    only = jnp.where(above, CLASSES - 1, HALF_CLASSES - 1).astype(jnp.int32)
    single = above | below
    alike = (first[:, None] == first[None, :]) & (first == last)[:, None] & (first == last)[None, :]
    fwd = jnp.where(active, jnp.where(single & alike, 1, 2), 0).astype(jnp.int32)
    bwd = jnp.where(active, jnp.where(single, 1, 2), 0).astype(jnp.int32)
    return fwd, bwd, only


def open_kernel(wq_ref, wk_ref, wv_ref, wo_ref, x_ref, gain_ref, posk_ref, posq_ref, segk_ref, segq_ref,
                qkv_ref, o_ref, normed_ref, idx_ref, fill_sem, sems):
    z, f = lax.axis_index('dp'), lax.axis_index('fsdp')
    D = wq_ref.shape[1]
    half = wq_ref.shape[0] // 2
    fills = [pltpu.make_async_copy(src, qkv_ref.at[f, :, pl.ds(n * D, D)], fill_sem.at[n]) for n, src in enumerate((wq_ref, wk_ref, wv_ref))]
    fills.append(pltpu.make_async_copy(wo_ref, o_ref.at[f], fill_sem.at[3]))
    for copy in fills:
        copy.start()
    barrier = pltpu.get_barrier_semaphore()
    for axis in 'cxy':
        pl.semaphore_signal(barrier, inc=1, device_id=partner_id(axis), device_id_type=pl.DeviceIdType.MESH)
    pl.semaphore_wait(barrier, 3)
    for copy in fills:
        copy.wait()

    def send(buf, n, shard, axis, rows=None):
        view = buf.at[shard] if rows is None else buf.at[shard, rows, :]
        copy = remote(view, view, sems, n, axis)
        copy.start()
        return copy

    bufs = (qkv_ref, o_ref)
    direct = {axis: [send(b, 8 * n + k, f, axis) for n, b in enumerate(bufs)] for k, axis in enumerate('xyc')}

    S = x_ref.shape[0]

    @pl.loop(0, S // 128)
    def _(i):
        rows = pl.ds(pl.multiple_of(i * 128, 128), 128)
        xf = x_ref[rows, :].astype(jnp.float32)
        inv = lax.rsqrt(jnp.mean(xf * xf, axis=1, keepdims=True) + EPSILON)
        normed_ref[rows, :] = (xf * inv * gain_ref[...]).astype(jnp.bfloat16)

    @pl.loop(0, S // 32)
    def _(i):
        rows = pl.ds(pl.multiple_of(i * 32, 32), 32)
        pk, sk = posk_ref[rows, :], segk_ref[rows, :]
        for n in range(S // LANES):
            cols = slice(n * LANES, (n + 1) * LANES)
            idx_ref[rows, cols] = class_index(posq_ref[0:1, cols], pk, segq_ref[0:1, cols], sk)

    for copy in direct['x']:
        copy.wait()
    along_y = [send(b, 8 * n + 3, f ^ 2, 'y', pl.ds(half, half)) for n, b in enumerate(bufs)]
    core_x = [send(b, 8 * n + 5, f ^ 2, 'c') for n, b in enumerate(bufs)]
    for copy in direct['y']:
        copy.wait()
    along_x = [send(b, 8 * n + 4, f ^ 4, 'x', pl.ds(0, half)) for n, b in enumerate(bufs)]
    core_y = [send(b, 8 * n + 6, f ^ 4, 'c') for n, b in enumerate(bufs)]
    for copy in along_y + along_x:
        copy.wait()
    core_d = [send(b, 8 * n + 7, f ^ 6, 'c') for n, b in enumerate(bufs)]
    for copy in direct['c'] + core_x + core_y + core_d:
        copy.wait()


def open_layer(wq_part, wk_part, wv_part, wo_part, x_row, gain, posk, posq, segk, segq):
    R, D = wq_part.shape
    S = x_row.shape[0]
    n = D // R
    vm = pl.BlockSpec(memory_space=pltpu.VMEM)
    w_qkv, w_o, normed, idx_t = pl.pallas_call(
        open_kernel,
        in_specs=[vm] * 10,
        out_specs=[vm] * 4,
        out_shape=[
            jax.ShapeDtypeStruct((n, R, 3 * D), jnp.bfloat16),
            jax.ShapeDtypeStruct((n, R, D), jnp.bfloat16),
            jax.ShapeDtypeStruct((S, D), jnp.bfloat16),
            jax.ShapeDtypeStruct((S, S), jnp.int32),
        ],
        scratch_shapes=[pltpu.SemaphoreType.DMA((4,)), pltpu.SemaphoreType.DMA((2, 16))],
        compiler_params=pltpu.CompilerParams(collective_id=2, has_side_effects=True),
        cost_estimate=pl.CostEstimate(flops=20_000_000_000, bytes_accessed=14_000_000, transcendentals=0),
        name="open_layer",
    )(wq_part, wk_part, wv_part, wo_part, x_row, gain.reshape(1, D), posk, posq, segk, segq)
    return w_qkv.reshape(D, 3 * D), w_o.reshape(D, D), normed, idx_t


def local_layer(x_in, positions, segments, rel_bias, gain_attn, gain_mlp, wq_part, wk_part, wv_part, wo_part, wi0_part, wi1_part, wf_part, grad_out):
    S, D = x_in.shape[1], x_in.shape[2]
    heads = rel_bias.shape[1]
    x_float = x_in[0].astype(jnp.float32)
    positions, segments, grad_out = positions[0], segments[0], grad_out[0]
    w_i0 = gather_full(wi0_part)
    w_i1 = gather_full(wi1_part)
    w_f = gather_full(wf_part)
    posk, posq = spread(positions)
    segk, segq = spread(segments)
    eq, ekt = place_onehots(positions)
    tab = bias_table(rel_bias)
    w_qkv, w_o, normed, idx_t = open_layer(wq_part, wk_part, wv_part, wo_part, x_in[0], gain_attn, posk, posq, segk, segq)
    qkv = project(normed, w_qkv).astype(jnp.bfloat16)
    fwd_mode, bwd_mode, only = block_modes(positions, segments, qkv, rel_bias)
    context, ctx32, probs = attn_fwd(qkv, idx_t, tab, tab[:, 0, :2 * CLASSES], fwd_mode, only)
    hidden = (x_float + project(context, w_o)).astype(jnp.bfloat16)
    h_float = hidden.astype(jnp.float32)
    mlp_in, norm2_pull = jax.vjp(rms_norm, h_float, gain_mlp)
    hidden_act, act_rel, d_gate, d_up = mlp_tiles(mlp_in, grad_out, w_i0, w_i1, w_f, relative_index('cxyz')[::2] // 2)

    ow, oi0, oi1 = 'cxyz', 'cyzx', 'czxy'
    half = act_rel.shape[1] // 2
    mlp_in_t = mlp_in.T
    kw, sw = product_t(act_rel[:, :half], grad_out), product_t(act_rel[:, half:], grad_out)
    k0, s0 = open_sum(relative_rows(mlp_in_t, oi0), d_gate)
    k1, s1 = open_sum(relative_rows(mlp_in_t, oi1), d_up)
    kw, sw = fold(kw, sw, ow[0])
    k0, s0 = fold(k0, s0, oi0[0])
    k1, s1 = fold(k1, s1, oi1[0])
    d_mlp_in = (project_t(d_gate, w_i0) + project_t(d_up, w_i1)).astype(jnp.bfloat16)
    d_h_norm, d_gain_mlp = norm2_pull(d_mlp_in)
    d_hidden = (grad_out.astype(jnp.float32) + d_h_norm).astype(jnp.bfloat16)
    oo = 'cxyz'
    ko, so = open_sum(relative_rows(context.T, oo), d_hidden)
    y_out = (h_float + project(hidden_act, w_f)).astype(jnp.bfloat16)
    d_context = project_t(d_hidden, w_o).astype(jnp.bfloat16)

    parts = []
    d_context, sw, s0, s1, so, y_out = together(d_context, sw, s0, s1, so, y_out)
    parts.append(attn_bwd(qkv, d_context, ctx32, probs, posk, posq, bwd_mode, only, eq, ekt, 0, 1))
    kw, sw = fold(kw, sw, ow[1])
    k0, s0 = fold(k0, s0, oi0[1])
    k1, s1 = fold(k1, s1, oi1[1])
    ko, so = fold(ko, so, oo[0])
    d_context, sw, s0, s1, so, head = together(d_context, sw, s0, s1, so, parts[0])
    parts[0] = head
    parts.append(attn_bwd(qkv, d_context, ctx32, probs, posk, posq, bwd_mode, only, eq, ekt, 1, 1))
    first_half, second_half = fold(kw, sw, ow[2])
    near = lax.axis_index('dp') == 0
    kw, sw = jnp.where(near, first_half, second_half), jnp.where(near, second_half, first_half)
    k0, s0 = fold(k0, s0, oi0[2])
    k1, s1 = fold(k1, s1, oi1[2])
    ko, so = fold(ko, so, oo[1])
    d_context, sw, s0, s1, so, head = together(d_context, sw, s0, s1, so, parts[1])
    parts[1] = head
    parts.append(attn_bwd(qkv, d_context, ctx32, probs, posk, posq, bwd_mode, only, eq, ekt, 2, 1))
    gw = kw + swap(sw, 'z')
    g0 = (k0 + swap(s0, oi0[3])).astype(jnp.bfloat16)
    g1 = (k1 + swap(s1, oi1[3])).astype(jnp.bfloat16)
    ko, so = fold(ko, so, oo[2])
    gw, g0, g1, so, head = together(gw, g0, g1, so, parts[2])
    parts[2] = head
    go = (ko + swap(so, oo[3])).astype(jnp.bfloat16)
    d_wf = close_sum(gw)
    grads = [[part[n] for part in parts] for n in range(3)]
    (d_wq, d_wk, d_wv, d_wi0, d_wi1, d_wo), small = tail_reduce(
        normed.T, x_in[0], w_qkv, grads, [part[3] for part in parts], d_gain_mlp.reshape(-1, LANES), (g0, g1, go))
    n_rows = D // LANES
    d_bias = small[:24].reshape(3, 8, LANES)[:, :HB, :CLASSES].reshape(heads, CLASSES).T
    return (y_out[None], d_bias, small[32:32 + n_rows].reshape(D), small[24:24 + n_rows].reshape(D),
            d_wq, d_wk, d_wv, d_wo, d_wi0, d_wi1, d_wf)


def solution(mesh):
    row_spec = P(ROW_AXES)
    whole = P()
    part_spec = P('fsdp')
    in_specs = (row_spec, row_spec, row_spec, whole, whole, whole) + (part_spec,) * 7 + (row_spec,)
    out_specs = (row_spec, whole, whole, whole) + (part_spec,) * 7
    return jax.shard_map(local_layer, mesh=mesh, in_specs=in_specs, out_specs=out_specs, check_vma=False)
```
